256 devices in a mesh: dp: 8 (over z_hi, core), tensor: 32 (over x, y, z_lo).
Axes of the slice: x: 4, y: 4, z: 8 (z_hi: 4, z_lo: 2; z = z_hi * 2 + z_lo), core: 2. Of those that a mesh axis runs over, the one named last changes fastest.
Arguments:
- inputs: bfloat16 [6144, 6144], P(('dp', 'tensor')), may hold values from -0.29882812 to 0.29882812
- norm_gain: float32 [6144], replicated, may hold values from 0.1 to 1.9
- norm_bias: float32 [6144], replicated, may hold values from -3 to 3
- query_grad: bfloat16 [6144, 12288], P('dp', 'tensor'), may hold values from -0.119628906 to 0.119628906
- stream_grad: bfloat16 [6144, 6144], P(('dp', 'tensor')), may hold values from -2.390625 to 2.390625
- query_weight: bfloat16 [6144, 12288], P(None, 'tensor'), may hold values from -0.0546875 to 0.0546875
Outputs:
- input_grad: bfloat16 [6144, 6144], P(('dp', 'tensor'))
- weight_grad: bfloat16 [6144, 12288], P(None, 'tensor')
The draws below stay inside these ranges and needn't reach their ends.
All inputs are finite; a program needn't handle non-finite values.
Results may differ from the reference program's by a relative error of at most 0.019.
Values may be sent and summed in bfloat16 or wider, within the bound.
A program may use at most 128 MiB of HBM per device.

```python
import jax
import jax.numpy as jnp
from jax import lax

D = 6144
HEADS = 96
HD = 128
TOK_DEV = 24
TOKENS = 6144
COLUMNS = 12288
N_DP = 8
N_TENSOR = 32


def strengthened(values, own_key, source, target, blocks, factor):
    owner, partner = [(jnp.arange(values.shape[axis_at]) // (values.shape[axis_at] // blocks)).reshape([-1 if axis == axis_at else 1 for axis in range(values.ndim)]) for axis_at in (source, target)]
    chosen = jax.random.permutation(own_key, blocks)[partner]
    strong = (owner == chosen) | (owner == (partner + blocks // 2) % blocks)
    return jnp.where(strong, factor * values, values)


def steps_of(rng, dims, cuts, low, high):
    def one(dim, shards_of):
        draws = jax.random.uniform(jax.random.fold_in(jax.random.fold_in(rng, 6), dim), (shards_of,), jnp.float32, low / len(cuts), high / len(cuts))
        return jnp.repeat(jnp.exp(draws), dims[dim] // shards_of).reshape((-1,) + (1,) * (len(dims) - dim - 1))

    factor_of = one(*cuts[0])
    for cut in cuts[1:]:
        factor_of = factor_of * one(*cut)
    return factor_of


def centred(own_key, shape, width, limit, cuts=(), kind=jnp.bfloat16):
    entries = jax.random.normal(own_key, shape, jnp.float32) * width
    if len(cuts) > 0:
        entries = steps_of(own_key, shape, cuts, -0.22, 0.18) * entries
    return jnp.clip(entries, min=-limit, max=limit).astype(kind)


def heavy_noise(stream_key, extent, scale, most, cuts, heavy, held_as=jnp.bfloat16):
    values = scale * jax.random.normal(stream_key, extent, jnp.float32)
    if cuts:
        values = values * steps_of(stream_key, extent, cuts, -0.22, 0.18)
    return jnp.clip(strengthened(values, jax.random.fold_in(stream_key, 3), *heavy), -most, most).astype(held_as)


def setup_inputs(seed: int = 0) -> dict:
    key_list = jax.random.split(jax.random.key(seed), 7)
    inputs = centred(key_list[0], (TOKENS, D), 0.05, 0.29882812, ((0, 256),))
    norm_gain = jnp.clip(1.0 + 0.18 * jax.random.normal(key_list[1], (D,), jnp.float32), 0.1, 1.9)
    norm_bias = centred(key_list[2], (D,), 0.5, 3.0, (), jnp.float32)
    query_grad = heavy_noise(key_list[3], (TOKENS, COLUMNS), 0.02, 0.119628906, ((0, 8), (1, 32)), (1, 0, 32, 2.75))
    stream_grad = centred(key_list[4], (TOKENS, D), 0.4, 2.390625, ((0, 256),))
    query_weight = centred(key_list[5], (D, COLUMNS), COLUMNS ** -0.5, 0.0546875, ((1, 32),))
    return {"inputs": inputs, "norm_gain": norm_gain, "norm_bias": norm_bias, "query_grad": query_grad, "stream_grad": stream_grad, "query_weight": query_weight}


epsilon = 1e-05

def normalize(values, norm_gain, norm_bias):
    as_float = values.astype(jnp.float32)
    centre = lax.optimization_barrier(jnp.mean(as_float, axis=-1, keepdims=True))
    offsets = as_float - centre
    variance = lax.optimization_barrier(jnp.mean(offsets * offsets, axis=-1, keepdims=True))
    inverse = lax.rsqrt(variance + epsilon)
    scaled = offsets * inverse
    normed = (scaled * norm_gain + norm_bias).astype(jnp.bfloat16)
    return (scaled, inverse, normed)

def norm_backward(scaled, inverse, normed_grad, norm_gain, stream_grad):
    weighted = normed_grad * norm_gain
    first_moment = lax.optimization_barrier(jnp.mean(weighted, axis=-1, keepdims=True))
    second_moment = lax.optimization_barrier(jnp.mean(weighted * scaled, axis=-1, keepdims=True))
    result = stream_grad.astype(jnp.float32) + inverse * (weighted - first_moment - scaled * second_moment)
    return result.astype(jnp.bfloat16)

def reference(inputs, norm_gain, norm_bias, query_grad, stream_grad, query_weight):
    per_group = TOK_DEV * N_TENSOR
    columns = HEADS * HD
    width_dev = columns // N_TENSOR
    grouped_in = inputs.reshape(N_DP, per_group, D)
    grouped_grad = query_grad.reshape(N_DP, per_group, columns)
    grouped_stream = stream_grad.reshape(N_DP, per_group, D)

    def group_step(carried, items):
        rows_in, rows_grad, rows_stream = items
        scaled, inverse, normed = normalize(rows_in, norm_gain, norm_bias)
        partial_value = jnp.dot(normed.T, rows_grad, preferred_element_type=jnp.float32)
        rounded = lax.optimization_barrier(partial_value.astype(jnp.bfloat16)).astype(jnp.float32)

        def add_block(running, block):
            begin = (block * width_dev).astype(jnp.int32)
            grad_cols = lax.dynamic_slice_in_dim(rows_grad, begin, width_dev, 1)
            weight_cols = lax.dynamic_slice_in_dim(query_weight, begin, width_dev, 1)
            term = lax.dot_general(grad_cols, weight_cols, (((1,), (1,)), ((), ())), preferred_element_type=jnp.float32)
            return (running + lax.optimization_barrier(term.astype(jnp.bfloat16)).astype(jnp.float32), None)
        normed_grad, _ = lax.scan(add_block, jnp.zeros((per_group, D), jnp.float32), jnp.arange(N_TENSOR, dtype=jnp.int32))
        grads_out = norm_backward(scaled, inverse, normed_grad, norm_gain, rows_stream)
        return (carried + rounded, grads_out)
    weight_grad, input_grad = lax.scan(group_step, jnp.zeros((D, columns), jnp.float32), (grouped_in, grouped_grad, grouped_stream))
    return (input_grad.reshape(N_DP * per_group, D), weight_grad.astype(jnp.bfloat16))
```

```python
import jax
import jax.numpy as jnp
from jax import lax
from jax.experimental import pallas as pl
from jax.experimental.pallas import tpu as pltpu
from jax.sharding import Mesh
from jax.sharding import PartitionSpec as P

MESH = pl.DeviceIdType.MESH
DP = ("zh", "c")
TENSOR = ("x", "y", "zl")
ALL = DP + TENSOR
EPS = 1e-05

F32 = jnp.float32
BF16 = jnp.bfloat16


def kernel(
    x_ref, gain_ref, bias_ref, q_ref, stream_ref, w_ref, dx_ref, dw_ref,
    scaled, inverse, normed, spread, own, xs, xt, qs, ws, wrelay, gs, rsb, fin, out,
    tsend, trecv, tsum, tzs, tzr, back, ngf,
    send_sem, recv_sem, local_sem,
):
    zh, c, x, y, zl = [lax.axis_index(name) for name in ALL]
    tok, width = x_ref.shape
    block = width // 8
    cols = q_ref.shape[1]
    rows_yz = 4 * tok
    group = 8 * rows_yz
    sub = block // 3
    quarter = block // 4

    def wrap(value):
        return lax.rem(value + 8, 4)

    xm, xp, xo = wrap(x - 1), wrap(x + 1), wrap(x + 2)
    ym, yp, yo = wrap(y - 1), wrap(y + 1), wrap(y + 2)
    zm, zp = wrap(zh - 1), wrap(zh + 1)
    other = 1 - c

    def at(offset, size, unit):
        return pl.ds(pl.multiple_of(offset, unit), size)

    copies = []
    locals_ = []

    def send(src, dst, **where):
        i = len(copies)
        copy = pltpu.make_async_remote_copy(
            src_ref=src,
            dst_ref=dst,
            send_sem=send_sem.at[i],
            recv_sem=recv_sem.at[i],
            device_id=where,
            device_id_type=MESH,
        )
        copy.start()
        copies.append(copy)
        return copy

    def local(src, dst):
        copy = pltpu.make_async_copy(src, dst, local_sem.at[len(locals_)])
        copy.start()
        locals_.append(copy)
        return copy

    pairs = [(dc, dx) for dc in range(2) for dx in range(4) if dc or dx]
    barrier = pltpu.get_barrier_semaphore()
    partners = [{"x": wrap(x + dx), "c": lax.rem(c + dc, 2)} for dc, dx in pairs]
    partners += [{"y": yp}, {"y": ym}, {"zl": 1 - zl}, {"zh": zp}, {"zh": zm}]
    for where in partners:
        pl.semaphore_signal(barrier, inc=1, device_id=where, device_id_type=MESH)

    mine = x * 2 + c
    q_local = local(q_ref, qs.at[0, c])
    w_local = local(w_ref.at[at(mine * block, block, block), :], ws.at[0])

    values = x_ref[...].astype(F32)
    centre = jnp.mean(values, axis=-1, keepdims=True)
    offsets = values - centre
    variance = jnp.mean(offsets * offsets, axis=-1, keepdims=True)
    inv = lax.rsqrt(variance + EPS)
    inverse[...] = jnp.broadcast_to(inv, inverse.shape)
    scaled[...] = offsets * inv
    normed[...] = (scaled[...] * gain_ref[...] + bias_ref[...]).astype(BF16)

    pl.semaphore_wait(barrier, len(partners))

    spread_in = []
    for dc, dx in pairs:
        tx, tc = wrap(x + dx), lax.rem(c + dc, 2)
        spread_in.append(
            send(normed.at[:, at((tx * 2 + tc) * block, block, 128)], spread.at[c * 4 + x], x=tx, c=tc)
        )
    q_d2d = {0: send(q_ref, qs.at[0, c], c=other)}
    q_down = send(q_ref, qs.at[1, c], x=xm)
    q_up = send(q_ref, qs.at[3, c], x=xp)

    spread[c * 4 + x] = normed[:, at(mine * block, block, 128)]
    for copy in spread_in:
        copy.wait_recv()
    for g in range(2):
        own[g] = jnp.concatenate([spread[g * 4 + i].astype(F32) for i in range(4)], axis=0).astype(BF16)
    base = y * 2 + zl
    own_in = local(own, xs.at[:, at(base * rows_yz, rows_yz, rows_yz), :])
    sl = [pl.ds(j * sub, sub) for j in range(3)]
    zl_in = [send(own.at[:, :, sl[j]], xs.at[:, at(base * rows_yz, rows_yz, rows_yz), sl[j]], zl=1 - zl) for j in range(3)]

    def w_rows(i, begin=0, size=block):
        return w_ref.at[at((i * 2 + c) * block + begin, size, size), :]

    w_down = send(w_rows(xm), ws.at[1], x=xm)
    w_up = send(w_rows(xp), ws.at[3], x=xp)
    half_w = block // 2
    w_relay_up = send(w_rows(xo, 0, half_w), wrelay.at[0], x=xp)
    w_relay_down = send(w_rows(xo, half_w, half_w), wrelay.at[1], x=xm)

    own_in.wait()
    y_up, y_down, relay_up, relay_down = {}, {}, {}, {}

    def y_rows(i):
        return at(i * 2 * rows_yz, 2 * rows_yz, 2 * rows_yz)

    def y_first(j):
        zl_in[j].wait_recv()
        piece = xs.at[:, y_rows(y), sl[j]]
        y_up[j] = send(piece, piece, y=yp)
        y_down[j] = send(piece, piece, y=ym)

    def y_relay(j):
        y_up[j].wait_recv()
        piece = xs.at[0, y_rows(ym), sl[j]]
        relay_up[j] = send(piece, piece, y=yp)
        y_down[j].wait_recv()
        piece = xs.at[1, y_rows(yp), sl[j]]
        relay_down[j] = send(piece, piece, y=ym)

    units = [(0, 0), (0, 1), (0, 2), (1, None), (3, None), (2, None)]

    def geometry(u):
        k, j = units[u]
        if j is None:
            return k, 0, quarter, 0
        return k, j * sub, sub // 4, j * (sub // 8)

    def g_rows(u, q, h):
        k, begin, step, _ = geometry(u)
        return at(begin + q * step + h * (step // 2), step // 2, 16)

    ring = {}

    def product(u):
        k, j = units[u]
        if j is not None:
            relay_up[j].wait_recv()
            relay_down[j].wait_recv()
            for g in range(2):
                xt[g, pl.ds(j * sub, sub), :] = xs[g, :, pl.ds(j * sub, sub)].T
            if j == 0:
                q_local.wait()
            if j == 0:
                q_d2d[0].wait_recv()
            pieces = [j * sub]
        else:
            q_d2d[k].wait_recv()
            pieces = [0, sub, 2 * sub]
        for begin in pieces:
            rows = pl.ds(begin, sub)
            gs[k, rows, :] = (
                jnp.dot(xt[0, rows, :], qs[k, 0], preferred_element_type=F32)
                + jnp.dot(xt[1, rows, :], qs[k, 1], preferred_element_type=F32)
            ).astype(BF16)

    def slot(u, d, s):
        k, _, step, r0 = geometry(u)
        return rsb.at[k, d, s, pl.ds(r0, step // 2), :]

    def rs_step(u, s):
        k = units[u][0]
        for d, (peer, sign) in enumerate(((zp, -1), (zm, 1))):
            if s == 0:
                ring[u, d, 0] = send(gs.at[k, g_rows(u, wrap(zh + sign), d), :], slot(u, d, 0), zh=peer)
                continue
            ring[u, d, s - 1].wait_recv()
            mine_part = gs[k, g_rows(u, wrap(zh + sign * (s + 1)), d), :].astype(F32)
            here = slot(u, d, s - 1)
            total = (here[...].astype(F32) + mine_part).astype(BF16)
            if s < 3:
                here[...] = total
                ring[u, d, s] = send(here, slot(u, d, s), zh=peer)
            elif k == 0:
                out[out_rows(u, 0, zh, d), :] = total
            else:
                fin[k, pl.ds(d * (quarter // 2), quarter // 2), :] = total
        if s == 3 and k:
            far = wrap(x + k)
            step = geometry(u)[2]
            ring[u, "x"] = send(fin.at[k], out.at[at(mine * block + zh * step, step, step), :], x=far)

    def source(k):
        return wrap(x - k) * 2 + c

    def out_rows(u, k, q, h):
        _, begin, step, _ = geometry(u)
        return at(source(k) * block + begin + q * step + h * (step // 2), step // 2, 16)

    def ag_step(u, s):
        k = units[u][0]
        if s == 0 and k:
            ring[u, "x"].wait_recv()
        for d, (peer, sign) in enumerate(((zp, -1), (zm, 1))):
            if s:
                ring[u, d, "a", s - 1].wait_recv()
            if s < 3:
                rows = out.at[out_rows(u, k, wrap(zh + sign * s), d), :]
                ring[u, d, "a", s] = send(rows, rows, zh=peer)
        if s == 3:
            size = sub if units[u][1] is not None else block
            begin = geometry(u)[1]
            whole = at(source(k) * block + begin, size, 16)
            ring[u, "c"] = send(out.at[whole, :], out.at[whole, :], c=other)
            local(out.at[whole, :], dw_ref.at[whole, :])

    def finish(u):
        k = units[u][0]
        ring[u, "c"].wait_recv()
        size = sub if units[u][1] is not None else block
        begin = geometry(u)[1]
        whole = at((wrap(x - k) * 2 + other) * block + begin, size, 16)
        local(out.at[whole, :], dw_ref.at[whole, :])

    q_relay = {}

    def q_forward():
        half = group // 2
        q_down.wait_recv()
        q_relay["down"] = send(qs.at[1, c, pl.ds(0, half), :], qs.at[2, c, pl.ds(0, half), :], x=xm)
        q_d2d[1] = send(qs.at[1, c], qs.at[1, c], c=other)
        q_up.wait_recv()
        q_relay["up"] = send(qs.at[3, c, pl.ds(half, half), :], qs.at[2, c, pl.ds(half, half), :], x=xp)
        q_d2d[3] = send(qs.at[3, c], qs.at[3, c], c=other)

    def q_last():
        q_relay["down"].wait_recv()
        q_relay["up"].wait_recv()
        q_d2d[2] = send(qs.at[2, c], qs.at[2, c], c=other)

    w_second = {}

    def w_forward():
        w_relay_up.wait_recv()
        w_second["up"] = send(wrelay.at[0], ws.at[2, pl.ds(0, half_w), :], x=xp)
        w_relay_down.wait_recv()
        w_second["down"] = send(wrelay.at[1], ws.at[2, pl.ds(half_w, half_w), :], x=xm)

    term_sent = {}

    def terms(dy):
        if dy == 2:
            w_local.wait()
            w_down.wait_recv()
            w_up.wait_recv()
            w_second["up"].wait_recv()
            w_second["down"].wait_recv()
        part = block // 3
        for g in range(2):
            for n in range(3):
                total = None
                for k in range(4):
                    piece = lax.dot_general(
                        qs[k, g, y_rows(wrap(y + dy)), :],
                        ws[k, pl.ds(n * part, part), :],
                        (((1,), (1,)), ((), ())),
                        preferred_element_type=F32,
                    )
                    total = piece if total is None else total + piece
                if dy:
                    tsend[dy - 1, g, :, pl.ds(n * part, part)] = total.astype(BF16)
                else:
                    tsum[g, :, pl.ds(n * part, part)] = total
        if dy == 2:
            term_sent["a0"] = send(tsend.at[1, 0], trecv.at[0], y=yp)
            term_sent["a1"] = send(tsend.at[1, 1], trecv.at[1], y=ym)
        elif dy == 1:
            term_sent["d1"] = send(tsend.at[0, 1], trecv.at[2], y=yp)
        elif dy == 3:
            term_sent["d0"] = send(tsend.at[2, 0], trecv.at[3], y=ym)

    def terms_relay():
        term_sent["a0"].wait_recv()
        trecv[0] = (trecv[0].astype(F32) + tsend[0, 0].astype(F32)).astype(BF16)
        term_sent["b0"] = send(trecv.at[0], trecv.at[4], y=yp)
        term_sent["a1"].wait_recv()
        trecv[1] = (trecv[1].astype(F32) + tsend[2, 1].astype(F32)).astype(BF16)
        term_sent["b1"] = send(trecv.at[1], trecv.at[5], y=ym)

    def half_rows(which):
        return at(which * rows_yz, rows_yz, rows_yz)

    def terms_sum():
        term_sent["b0"].wait_recv()
        term_sent["d0"].wait_recv()
        term_sent["b1"].wait_recv()
        term_sent["d1"].wait_recv()
        for g, (i, j) in enumerate(((4, 3), (5, 2))):
            far = half_rows(1 - zl)
            tzs[g] = (tsum[g, far, :] + trecv[i, far, :].astype(F32) + trecv[j, far, :].astype(F32)).astype(BF16)
        term_sent["z"] = send(tzs, tzr, zl=1 - zl)

    def terms_back():
        term_sent["z"].wait_recv()
        for g, (i, j) in enumerate(((4, 3), (5, 2))):
            near = half_rows(zl)
            total = (
                tsum[g, near, :]
                + trecv[i, near, :].astype(F32)
                + trecv[j, near, :].astype(F32)
                + tzr[g].astype(F32)
            )
            for i in range(4):
                back[g * 4 + i] = total[i * tok : (i + 1) * tok, :].astype(BF16)
        for dc, dx in pairs:
            tx, tc = wrap(x + dx), lax.rem(c + dc, 2)
            term_sent[dc, dx] = send(back.at[tc * 4 + tx], ngf.at[mine], x=tx, c=tc)
        ngf[mine] = back[c * 4 + x]

    def norm_backward():
        for pair in pairs:
            term_sent[pair].wait_recv()
        grad = jnp.concatenate([ngf[i].astype(F32) for i in range(8)], axis=1)
        weighted = grad * gain_ref[...]
        scaled_now = scaled[...]
        first = jnp.mean(weighted, axis=-1, keepdims=True)
        second = jnp.mean(weighted * scaled_now, axis=-1, keepdims=True)
        result = stream_ref[...].astype(F32) + inverse[:, 0:1] * (weighted - first - scaled_now * second)
        dx_ref[...] = result.astype(BF16)

    stages = [
        lambda u: (product(u), rs_step(u, 0)),
        lambda u: rs_step(u, 1),
        lambda u: rs_step(u, 2),
        lambda u: rs_step(u, 3),
        lambda u: ag_step(u, 0),
        lambda u: ag_step(u, 1),
        lambda u: ag_step(u, 2),
        lambda u: ag_step(u, 3),
        finish,
    ]
    start = [0, 1, 2, 4, 6, 8]
    before = {
        0: [lambda: y_first(0), lambda: y_first(1), lambda: y_first(2), lambda: y_relay(0), lambda: y_relay(1)],
        1: [lambda: y_relay(2)],
        2: [q_forward],
        5: [w_forward],
        7: [q_last],
    }
    after = {
        8: [lambda: terms(2)],
        9: [lambda: terms(1), lambda: terms(3)],
        10: [terms_relay, lambda: terms(0)],
        12: [terms_sum],
        13: [terms_back],
        14: [norm_backward],
    }
    for tick in range(start[-1] + len(stages)):
        for action in before.get(tick, []):
            action()
        for u in range(len(units)):
            if 0 <= tick - start[u] < len(stages):
                stages[tick - start[u]](u)
        for action in after.get(tick, []):
            action()

    for copy in copies:
        copy.wait_send()
    for copy in locals_:
        if all(copy is not done for done in (q_local, w_local, own_in)):
            copy.wait()


N_COPIES = 140
N_LOCAL = 16


def shards(inputs, norm_gain, norm_bias, query_grad, stream_grad, query_weight):
    tok, width = inputs.shape
    rows, cols = query_grad.shape
    block = width // 8
    ordered = query_grad.reshape(4, 4, 2, tok, cols).transpose(1, 2, 0, 3, 4).reshape(rows, cols)
    vmem = pl.BlockSpec(memory_space=pltpu.VMEM)
    hbm = pl.BlockSpec(memory_space=pltpu.HBM)
    return pl.pallas_call(
        kernel,
        out_shape=(
            jax.ShapeDtypeStruct((tok, width), BF16),
            jax.ShapeDtypeStruct((width, cols), BF16),
        ),
        in_specs=[vmem, vmem, vmem, vmem, vmem, hbm],
        out_specs=(vmem, hbm),
        scratch_shapes=[
            pltpu.VMEM((tok, width), F32),
            pltpu.VMEM((tok, 128), F32),
            pltpu.VMEM((tok, width), BF16),
            pltpu.VMEM((8, tok, block), BF16),
            pltpu.VMEM((2, 4 * tok, block), BF16),
            pltpu.VMEM((2, rows, block), BF16),
            pltpu.VMEM((2, block, rows), BF16),
            pltpu.VMEM((4, 2, rows, cols), BF16),
            pltpu.VMEM((4, block, cols), BF16),
            pltpu.VMEM((2, block // 2, cols), BF16),
            pltpu.VMEM((4, block, cols), BF16),
            pltpu.VMEM((4, 2, 3, block // 8, cols), BF16),
            pltpu.VMEM((4, block // 4, cols), BF16),
            pltpu.VMEM((width, cols), BF16),
            pltpu.VMEM((3, 2, 8 * tok, block), BF16),
            pltpu.VMEM((6, 8 * tok, block), BF16),
            pltpu.VMEM((2, 8 * tok, block), F32),
            pltpu.VMEM((2, 4 * tok, block), BF16),
            pltpu.VMEM((2, 4 * tok, block), BF16),
            pltpu.VMEM((8, tok, block), BF16),
            pltpu.VMEM((8, tok, block), BF16),
            pltpu.SemaphoreType.DMA((N_COPIES,)),
            pltpu.SemaphoreType.DMA((N_COPIES,)),
            pltpu.SemaphoreType.DMA((N_LOCAL,)),
        ],
        compiler_params=pltpu.CompilerParams(
            collective_id=0, has_side_effects=True, vmem_limit_bytes=60 * 1024 * 1024
        ),
    )(inputs, norm_gain.reshape(1, width), norm_bias.reshape(1, width), ordered, stream_grad, query_weight)


def solution(mesh):
    torus = Mesh(mesh.devices.reshape(4, 2, 4, 4, 2), ALL)
    return jax.shard_map(
        shards,
        mesh=torus,
        in_specs=(P(ALL, None), P(), P(), P(DP, TENSOR), P(ALL, None), P(None, TENSOR)),
        out_specs=(P(ALL, None), P(None, TENSOR)),
        check_vma=False,
    )
```

```python
import jax
import jax.numpy as jnp
from jax import lax
from jax.experimental import pallas as pl
from jax.experimental.pallas import tpu as pltpu
from jax.sharding import Mesh
from jax.sharding import PartitionSpec as P

MESH = pl.DeviceIdType.MESH
DP = ("zh", "c")
TENSOR = ("x", "y", "zl")
ALL = DP + TENSOR
EPS = 1e-05

F32 = jnp.float32
BF16 = jnp.bfloat16


def kernel(
    x_ref, gain_ref, bias_ref, q_ref, stream_ref, w_ref, dx_ref, out,
    scaled, inverse, normed, spread, own, xs, xt, qs, ws, wrelay, gs, rsb, fin,
    tsend, trecv, tsum, tzs, tzr, back, ngf,
    send_sem, recv_sem, local_sem,
):
    zh, c, x, y, zl = [lax.axis_index(name) for name in ALL]
    tok, width = x_ref.shape
    block = width // 8
    cols = q_ref.shape[1]
    rows_yz = 4 * tok
    group = 8 * rows_yz
    sixth = block // 6
    bounds = [(0, sixth), (sixth, sixth), (2 * sixth, 2 * sixth), (4 * sixth, 2 * sixth)]
    sl = [pl.ds(*bound) for bound in bounds]

    def wrap(value):
        return lax.rem(value + 8, 4)

    xm, xp, xo = wrap(x - 1), wrap(x + 1), wrap(x + 2)
    ym, yp, yo = wrap(y - 1), wrap(y + 1), wrap(y + 2)
    zm, zp = wrap(zh - 1), wrap(zh + 1)
    other = 1 - c

    def at(offset, size, unit):
        return pl.ds(pl.multiple_of(offset, unit), size)

    copies = []
    locals_ = []

    def send(src, dst, **where):
        i = len(copies)
        copy = pltpu.make_async_remote_copy(
            src_ref=src,
            dst_ref=dst,
            send_sem=send_sem.at[i],
            recv_sem=recv_sem.at[i],
            device_id=where,
            device_id_type=MESH,
        )
        copy.start()
        copies.append(copy)
        return copy

    def local(src, dst):
        copy = pltpu.make_async_copy(src, dst, local_sem.at[len(locals_)])
        copy.start()
        locals_.append(copy)
        return copy

    pairs = [(dc, dx) for dc in range(2) for dx in range(4) if dc or dx]
    barrier = pltpu.get_barrier_semaphore()
    partners = [{"x": wrap(x + dx), "c": lax.rem(c + dc, 2)} for dc, dx in pairs]
    partners += [{"y": yp}, {"y": ym}, {"zl": 1 - zl}, {"zh": zp}, {"zh": zm}]
    for where in partners:
        pl.semaphore_signal(barrier, inc=1, device_id=where, device_id_type=MESH)

    mine = x * 2 + c
    w_local = local(w_ref.at[at(mine * block, block, block), :], ws.at[0])

    values = x_ref[...].astype(F32)
    centre = jnp.mean(values, axis=-1, keepdims=True)
    offsets = values - centre
    variance = jnp.mean(offsets * offsets, axis=-1, keepdims=True)
    inv = lax.rsqrt(variance + EPS)
    inverse[...] = jnp.broadcast_to(inv, inverse.shape)
    scaled[...] = offsets * inv
    normed[...] = (scaled[...] * gain_ref[...] + bias_ref[...]).astype(BF16)

    pl.semaphore_wait(barrier, len(partners))

    chunks = [(0, sixth), (sixth, 5 * sixth)]
    spread_in = []
    for begin, size in chunks:
        for dc, dx in pairs:
            tx, tc = wrap(x + dx), lax.rem(c + dc, 2)
            piece = normed.at[:, at((tx * 2 + tc) * block + begin, size, 128)]
            spread_in.append(send(piece, spread.at[c * 4 + x, :, pl.ds(begin, size)], x=tx, c=tc))

    for i in range(8):
        parts = [q_ref[(g * 8 + i) * tok : (g * 8 + i + 1) * tok, :].astype(F32) for g in range(4)]
        qs[0, c, i * rows_yz : (i + 1) * rows_yz, :] = jnp.concatenate(parts, axis=0).astype(BF16)
    q_d2d = {0: send(qs.at[0, c], qs.at[0, c], c=other)}
    q_down = send(qs.at[0, c], qs.at[1, c], x=xm)
    q_up = send(qs.at[0, c], qs.at[3, c], x=xp)

    spread[c * 4 + x] = normed[:, at(mine * block, block, 128)]
    base = y * 2 + zl
    own_in, zl_in = [], []
    for i, (begin, size) in enumerate(chunks):
        for copy in spread_in[i * len(pairs) : (i + 1) * len(pairs)]:
            copy.wait_recv()
        cut = pl.ds(begin, size)
        for g in range(2):
            parts = [spread[g * 4 + n, :, cut].astype(F32) for n in range(4)]
            own[g, :, cut] = jnp.concatenate(parts, axis=0).astype(BF16)
        own_in.append(local(own.at[:, :, cut], xs.at[:, at(base * rows_yz, rows_yz, rows_yz), cut]))
        for first, count in bounds:
            if begin <= first < begin + size:
                cut = pl.ds(first, count)
                zl_in.append(send(own.at[:, :, cut], xs.at[:, at(base * rows_yz, rows_yz, rows_yz), cut], zl=1 - zl))

    def w_rows(i, begin=0, size=block):
        return w_ref.at[at((i * 2 + c) * block + begin, size, size), :]

    w_down = send(w_rows(xm), ws.at[1], x=xm)
    w_up = send(w_rows(xp), ws.at[3], x=xp)
    half_w = block // 2

    y_up, y_down, relay_up, relay_down = {}, {}, {}, {}

    def y_rows(i):
        return at(i * 2 * rows_yz, 2 * rows_yz, 2 * rows_yz)

    def y_first(j):
        if j < 2:
            own_in[j].wait()
        zl_in[j].wait_recv()
        piece = xs.at[:, y_rows(y), sl[j]]
        y_up[j] = send(piece, piece, y=yp)
        y_down[j] = send(piece, piece, y=ym)

    def y_relay_up(j):
        y_up[j].wait_recv()
        piece = xs.at[0, y_rows(ym), sl[j]]
        relay_up[j] = send(piece, piece, y=yp)

    def y_relay_down(j):
        y_down[j].wait_recv()
        piece = xs.at[1, y_rows(yp), sl[j]]
        relay_down[j] = send(piece, piece, y=ym)

    units = [(k, first * sixth, size * sixth) for k, first, size in UNITS]

    def rows_of(u, q, h, base=0):
        _, begin, size = units[u]
        return at(base + begin + q * (size // 4) + h * (size // 8), size // 8, 16)

    ring = {}

    def prepare(j):
        begin, size = bounds[j]
        if not j:
            q_d2d[0].wait_recv()
        relay_up[j].wait_recv()
        relay_down[j].wait_recv()
        for g in range(2):
            xt[g, pl.ds(begin, size), :] = xs[g, :, pl.ds(begin, size)].T

    arrived = []

    def product(u):
        k, begin, size = units[u]
        if k and k not in arrived:
            arrived.append(k)
            q_d2d[k].wait_recv()
        piece = min(size, 2 * sixth)
        if size % piece:
            piece = sixth
        for first in range(begin, begin + size, piece):
            rows = pl.ds(first, piece)
            gs[k, rows, :] = (
                jnp.dot(xt[0, rows, :], qs[k, 0], preferred_element_type=F32)
                + jnp.dot(xt[1, rows, :], qs[k, 1], preferred_element_type=F32)
            ).astype(BF16)
        for d in range(2):
            ring[u, d, 0] = send(gs.at[k, rows_of(u, wrap(zh + (-1, 1)[d]), d), :], slot(u, d, 0), zh=(zp, zm)[d])

    def slot(u, d, s):
        k, begin, size = units[u]
        return rsb.at[k, d, s, pl.ds(begin // 8, size // 8), :]

    def source(k):
        return wrap(x - k) * 2 + c

    def rs_step(u, s, d):
        k, begin, size = units[u]
        ring[u, d, s - 1].wait_recv()
        sign = (-1, 1)[d]
        mine_part = gs[k, rows_of(u, wrap(zh + sign * (s + 1)), d), :].astype(F32)
        here = slot(u, d, s - 1)
        total = (here[...].astype(F32) + mine_part).astype(BF16)
        if s < 3:
            here[...] = total
            ring[u, d, s] = send(here, slot(u, d, s), zh=(zp, zm)[d])
        elif k == 0:
            out[rows_of(u, zh, d, mine * block), :] = total
        else:
            fin[k, pl.ds(begin // 4 + d * (size // 8), size // 8), :] = total

    def across(u):
        k, begin, size = units[u]
        landing = at(mine * block + begin + zh * (size // 4), size // 4, 32)
        ring[u, "x"] = send(fin.at[k, pl.ds(begin // 4, size // 4), :], out.at[landing, :], x=wrap(x + k))

    crossed = []

    def ag_step(u, s, d):
        k, begin, size = units[u]
        if s:
            ring[u, d, "a", s - 1].wait_recv()
        elif k and u not in crossed:
            crossed.append(u)
            ring[u, "x"].wait_recv()
        rows = out.at[rows_of(u, wrap(zh + (-1, 1)[d] * s), d, source(k) * block), :]
        ring[u, d, "a", s] = send(rows, rows, zh=(zp, zm)[d])

    def to_partner(u):
        k, begin, size = units[u]
        for d in range(2):
            ring[u, d, "a", 2].wait_recv()
        whole = at(source(k) * block + begin, size, 128)
        ring[u, "c"] = send(out.at[whole, :], out.at[whole, :], c=other)

    def finish(u):
        ring[u, "c"].wait_recv()

    q_relay, w_relay = {}, {}

    half = group // 2

    def q_forward_down():
        q_down.wait_recv()
        q_relay["down"] = send(qs.at[1, c, pl.ds(0, half), :], qs.at[2, c, pl.ds(0, half), :], x=xm)
        q_d2d[1] = send(qs.at[1, c], qs.at[1, c], c=other)

    def q_forward_up():
        q_up.wait_recv()
        q_relay["up"] = send(qs.at[3, c, pl.ds(half, half), :], qs.at[2, c, pl.ds(half, half), :], x=xp)
        q_d2d[3] = send(qs.at[3, c], qs.at[3, c], c=other)

    def w_first():
        w_relay["up"] = send(w_rows(xo, 0, half_w), wrelay.at[0], x=xp)
        w_relay["down"] = send(w_rows(xo, half_w, half_w), wrelay.at[1], x=xm)

    def q_last():
        q_relay["down"].wait_recv()
        q_relay["up"].wait_recv()
        q_d2d[2] = send(qs.at[2, c], qs.at[2, c], c=other)

    w_second = {}

    def w_forward_up():
        w_relay["up"].wait_recv()
        w_second["up"] = send(wrelay.at[0], ws.at[2, pl.ds(0, half_w), :], x=xp)

    def w_forward_down():
        w_relay["down"].wait_recv()
        w_second["down"] = send(wrelay.at[1], ws.at[2, pl.ds(half_w, half_w), :], x=xm)

    term_sent = {}

    def terms(dy):
        if dy == 2:
            w_local.wait()
            w_down.wait_recv()
            w_up.wait_recv()
            w_second["up"].wait_recv()
            w_second["down"].wait_recv()
        part = block // 3
        for g in range(2):
            for n in range(3):
                total = None
                for k in range(4):
                    piece = lax.dot_general(
                        qs[k, g, y_rows(wrap(y + dy)), :],
                        ws[k, pl.ds(n * part, part), :],
                        (((1,), (1,)), ((), ())),
                        preferred_element_type=F32,
                    )
                    total = piece if total is None else total + piece
                if dy:
                    tsend[dy - 1, g, :, pl.ds(n * part, part)] = total.astype(BF16)
                else:
                    tsum[g, :, pl.ds(n * part, part)] = total
        if dy == 2:
            term_sent["a0"] = send(tsend.at[1, 0], trecv.at[0], y=yp)
            term_sent["a1"] = send(tsend.at[1, 1], trecv.at[1], y=ym)
        elif dy == 1:
            term_sent["d1"] = send(tsend.at[0, 1], trecv.at[2], y=yp)
        elif dy == 3:
            term_sent["d0"] = send(tsend.at[2, 0], trecv.at[3], y=ym)

    def terms_relay_up():
        term_sent["a0"].wait_recv()
        trecv[0] = (trecv[0].astype(F32) + tsend[0, 0].astype(F32)).astype(BF16)
        term_sent["b0"] = send(trecv.at[0], trecv.at[4], y=yp)

    def terms_relay_down():
        term_sent["a1"].wait_recv()
        trecv[1] = (trecv[1].astype(F32) + tsend[2, 1].astype(F32)).astype(BF16)
        term_sent["b1"] = send(trecv.at[1], trecv.at[5], y=ym)

    def half_rows(which):
        return at(which * rows_yz, rows_yz, rows_yz)

    def terms_sum():
        term_sent["b0"].wait_recv()
        term_sent["d0"].wait_recv()
        term_sent["b1"].wait_recv()
        term_sent["d1"].wait_recv()
        for g, (i, j) in enumerate(((4, 3), (5, 2))):
            far = half_rows(1 - zl)
            tzs[g] = (tsum[g, far, :] + trecv[i, far, :].astype(F32) + trecv[j, far, :].astype(F32)).astype(BF16)
        term_sent["z"] = send(tzs, tzr, zl=1 - zl)

    def terms_back():
        term_sent["z"].wait_recv()
        for g, (i, j) in enumerate(((4, 3), (5, 2))):
            near = half_rows(zl)
            total = (
                tsum[g, near, :]
                + trecv[i, near, :].astype(F32)
                + trecv[j, near, :].astype(F32)
                + tzr[g].astype(F32)
            )
            for i in range(4):
                back[g * 4 + i] = total[i * tok : (i + 1) * tok, :].astype(BF16)
        for dc, dx in pairs:
            tx, tc = wrap(x + dx), lax.rem(c + dc, 2)
            term_sent[dc, dx] = send(back.at[tc * 4 + tx], ngf.at[mine], x=tx, c=tc)
        ngf[mine] = back[c * 4 + x]

    def norm_backward():
        for pair in pairs:
            term_sent[pair].wait_recv()
        grad = jnp.concatenate([ngf[i].astype(F32) for i in range(8)], axis=1)
        weighted = grad * gain_ref[...]
        scaled_now = scaled[...]
        first = jnp.mean(weighted, axis=-1, keepdims=True)
        second = jnp.mean(weighted * scaled_now, axis=-1, keepdims=True)
        result = stream_ref[...].astype(F32) + inverse[:, 0:1] * (weighted - first - scaled_now * second)
        dx_ref[...] = result.astype(BF16)

    actions = {
        "yf": y_first, "yu": y_relay_up, "yd": y_relay_down, "prep": prepare, "P": product, "R": rs_step,
        "X": across, "A": ag_step, "D": to_partner, "F": finish, "qd": q_forward_down, "qu": q_forward_up,
        "ql": q_last, "wr": w_first, "wfu": w_forward_up, "wfd": w_forward_down, "T": terms,
        "tr0": terms_relay_up, "tr1": terms_relay_down, "ts": terms_sum, "tb": terms_back, "nb": norm_backward,
    }
    for name, *rest in ORDER:
        actions[name](*rest)

    for copy in copies:
        copy.wait_send()


N_COPIES = 224
N_LOCAL = 8

ORDER = [
    ("yf", 0), ("yf", 1), ("yf", 2), ("yu", 0), ("yd", 0), ("yf", 3), ("yu", 1), ("yd", 1), ("qd",), ("qu",),
    ("wr",), ("yu", 2), ("yd", 2), ("prep", 0), ("P", 0), ("R", 0, 1, 0), ("yu", 3), ("yd", 3), ("R", 0, 1, 1),
    ("prep", 1), ("P", 1), ("P", 2), ("P", 3), ("prep", 2), ("P", 4), ("R", 0, 2, 0), ("R", 0, 2, 1), ("R", 1, 1, 0),
    ("prep", 3), ("P", 5), ("P", 6), ("P", 7), ("R", 1, 1, 1), ("R", 2, 1, 0), ("R", 2, 1, 1), ("R", 3, 1, 0),
    ("R", 3, 1, 1), ("R", 4, 1, 0), ("R", 4, 1, 1), ("R", 1, 2, 0), ("R", 0, 3, 0), ("R", 0, 3, 1), ("R", 5, 1, 0),
    ("R", 5, 1, 1), ("A", 0, 0, 0), ("A", 0, 0, 1), ("ql",), ("R", 6, 1, 0), ("R", 6, 1, 1), ("P", 8), ("P", 9),
    ("R", 7, 1, 0), ("R", 7, 1, 1), ("R", 1, 2, 1), ("R", 2, 2, 0), ("R", 2, 2, 1), ("R", 3, 2, 0), ("R", 3, 2, 1),
    ("R", 4, 2, 0), ("wfu",), ("wfd",), ("R", 4, 2, 1), ("R", 1, 3, 0), ("R", 5, 2, 0), ("R", 5, 2, 1),
    ("A", 0, 1, 0), ("A", 0, 1, 1), ("R", 6, 2, 0), ("R", 6, 2, 1), ("R", 8, 1, 0), ("R", 8, 1, 1), ("R", 9, 1, 0),
    ("R", 9, 1, 1), ("T", 2), ("T", 1), ("T", 3), ("T", 0), ("R", 7, 2, 0), ("R", 7, 2, 1), ("R", 1, 3, 1),
    ("R", 2, 3, 0), ("R", 2, 3, 1), ("X", 2), ("R", 3, 3, 0), ("R", 3, 3, 1), ("X", 3), ("R", 4, 3, 0),
    ("R", 4, 3, 1), ("R", 5, 3, 0), ("R", 5, 3, 1), ("R", 6, 3, 0), ("R", 6, 3, 1), ("R", 8, 2, 0), ("X", 6),
    ("A", 1, 0, 0), ("A", 1, 0, 1), ("A", 4, 0, 0), ("R", 8, 2, 1), ("tr0",), ("tr1",), ("A", 4, 0, 1),
    ("A", 5, 0, 0), ("A", 5, 0, 1), ("A", 0, 2, 0), ("A", 0, 2, 1), ("R", 9, 2, 0), ("A", 2, 0, 0), ("A", 2, 0, 1),
    ("A", 3, 0, 0), ("R", 9, 2, 1), ("A", 3, 0, 1), ("R", 7, 3, 0), ("R", 7, 3, 1), ("X", 7), ("A", 6, 0, 0),
    ("A", 6, 0, 1), ("A", 1, 1, 1), ("R", 8, 3, 0), ("A", 1, 1, 0), ("R", 8, 3, 1), ("X", 8), ("A", 4, 1, 0),
    ("A", 4, 1, 1), ("A", 5, 1, 0), ("A", 5, 1, 1), ("A", 7, 0, 0), ("A", 7, 0, 1), ("D", 0), ("R", 9, 3, 0),
    ("A", 2, 1, 1), ("F", 0), ("A", 8, 0, 0), ("A", 8, 0, 1), ("A", 2, 1, 0), ("R", 9, 3, 1), ("X", 9),
    ("A", 3, 1, 0), ("A", 3, 1, 1), ("ts",), ("A", 6, 1, 0), ("A", 6, 1, 1), ("A", 1, 2, 0), ("A", 1, 2, 1),
    ("A", 4, 2, 0), ("A", 9, 0, 0), ("A", 9, 0, 1), ("A", 4, 2, 1), ("A", 5, 2, 0), ("A", 5, 2, 1), ("A", 7, 1, 0),
    ("A", 7, 1, 1), ("A", 8, 1, 0), ("A", 2, 2, 1), ("A", 2, 2, 0), ("A", 8, 1, 1), ("A", 3, 2, 0), ("A", 3, 2, 1),
    ("A", 6, 2, 1), ("A", 9, 1, 1), ("tb",), ("A", 6, 2, 0), ("A", 7, 2, 1), ("D", 1), ("D", 4), ("F", 1), ("F", 4),
    ("A", 9, 1, 0), ("A", 8, 2, 1), ("nb",), ("D", 5), ("F", 5), ("A", 7, 2, 0), ("A", 8, 2, 0), ("A", 9, 2, 1),
    ("D", 2), ("D", 3), ("F", 2), ("F", 3), ("D", 6), ("A", 9, 2, 0), ("F", 6), ("D", 7), ("D", 8), ("F", 7),
    ("F", 8), ("D", 9), ("F", 9),
]
UNITS = [(0, 0, 1), (0, 1, 1), (1, 0, 2), (3, 0, 2), (0, 2, 2), (0, 4, 2), (1, 2, 4), (3, 2, 4), (2, 0, 3), (2, 3, 3)]


def shards(inputs, norm_gain, norm_bias, query_grad, stream_grad, query_weight):
    tok, width = inputs.shape
    rows, cols = query_grad.shape
    block = width // 8
    vmem = pl.BlockSpec(memory_space=pltpu.VMEM)
    hbm = pl.BlockSpec(memory_space=pltpu.HBM)
    return pl.pallas_call(
        kernel,
        out_shape=(
            jax.ShapeDtypeStruct((tok, width), BF16),
            jax.ShapeDtypeStruct((width, cols), BF16),
        ),
        in_specs=[vmem, vmem, vmem, vmem, vmem, hbm],
        out_specs=(vmem, vmem),
        scratch_shapes=[
            pltpu.VMEM((tok, width), F32),
            pltpu.VMEM((tok, 128), F32),
            pltpu.VMEM((tok, width), BF16),
            pltpu.VMEM((8, tok, block), BF16),
            pltpu.VMEM((2, 4 * tok, block), BF16),
            pltpu.VMEM((2, rows, block), BF16),
            pltpu.VMEM((2, block, rows), BF16),
            pltpu.VMEM((4, 2, rows, cols), BF16),
            pltpu.VMEM((4, block, cols), BF16),
            pltpu.VMEM((2, block // 2, cols), BF16),
            pltpu.VMEM((4, block, cols), BF16),
            pltpu.VMEM((4, 2, 3, block // 8, cols), BF16),
            pltpu.VMEM((4, block // 4, cols), BF16),
            pltpu.VMEM((3, 2, 8 * tok, block), BF16),
            pltpu.VMEM((6, 8 * tok, block), BF16),
            pltpu.VMEM((2, 8 * tok, block), F32),
            pltpu.VMEM((2, 4 * tok, block), BF16),
            pltpu.VMEM((2, 4 * tok, block), BF16),
            pltpu.VMEM((8, tok, block), BF16),
            pltpu.VMEM((8, tok, block), BF16),
            pltpu.SemaphoreType.DMA((N_COPIES,)),
            pltpu.SemaphoreType.DMA((N_COPIES,)),
            pltpu.SemaphoreType.DMA((N_LOCAL,)),
        ],
        compiler_params=pltpu.CompilerParams(
            collective_id=0, has_side_effects=True, vmem_limit_bytes=44 * 1024 * 1024
        ),
    )(inputs, norm_gain.reshape(1, width), norm_bias.reshape(1, width), query_grad, stream_grad, query_weight)


def solution(mesh):
    torus = Mesh(mesh.devices.reshape(4, 2, 4, 4, 2), ALL)
    return jax.shard_map(
        shards,
        mesh=torus,
        in_specs=(P(ALL, None), P(), P(), P(DP, TENSOR), P(ALL, None), P(None, TENSOR)),
        out_specs=(P(ALL, None), P(None, TENSOR)),
        check_vma=False,
    )
```

```python
import jax
import jax.numpy as jnp
from jax import lax
from jax.experimental import pallas as pl
from jax.experimental.pallas import tpu as pltpu
from jax.sharding import Mesh
from jax.sharding import PartitionSpec as P

MESH = pl.DeviceIdType.MESH
DP = ("zh", "c")
TENSOR = ("x", "y", "zl")
ALL = DP + TENSOR
EPS = 1e-05

F32 = jnp.float32
BF16 = jnp.bfloat16


def kernel(
    x_hbm, gain_hbm, bias_hbm, q_hbm, stream_hbm, w_ref, dx_ref, out,
    x_ref, gain_ref, bias_ref, q_ref, stream_ref,
    scaled, inverse, normed, spread, own, xs, xt, qs, ws, wrelay, gs, rsb, fin,
    tsend, trecv, tsum, tzs, tzr, back, ngf,
    send_sem, recv_sem, local_sem,
):
    zh, c, x, y, zl = [lax.axis_index(name) for name in ALL]
    tok, width = x_ref.shape
    block = width // 8
    cols = q_ref.shape[1]
    rows_yz = 4 * tok
    group = 8 * rows_yz
    sixth = block // 6
    bounds = [(i * sixth, sixth) for i in range(6)]
    sl = [pl.ds(*bound) for bound in bounds]

    def wrap(value):
        return lax.rem(value + 8, 4)

    xm, xp, xo = wrap(x - 1), wrap(x + 1), wrap(x + 2)
    ym, yp, yo = wrap(y - 1), wrap(y + 1), wrap(y + 2)
    zm, zp = wrap(zh - 1), wrap(zh + 1)
    other = 1 - c

    def at(offset, size, unit):
        return pl.ds(pl.multiple_of(offset, unit), size)

    copies = []
    locals_ = []

    def send(src, dst, **where):
        i = len(copies)
        copy = pltpu.make_async_remote_copy(
            src_ref=src,
            dst_ref=dst,
            send_sem=send_sem.at[i],
            recv_sem=recv_sem.at[i],
            device_id=where,
            device_id_type=MESH,
        )
        copy.start()
        copies.append(copy)
        return copy

    def local(src, dst):
        copy = pltpu.make_async_copy(src, dst, local_sem.at[len(locals_)])
        copy.start()
        locals_.append(copy)
        return copy

    first_loads = [local(x_hbm, x_ref), local(gain_hbm, gain_ref), local(bias_hbm, bias_ref)]

    pairs = [(dc, dx) for dc in range(2) for dx in range(4) if dc or dx]
    barrier = pltpu.get_barrier_semaphore()
    partners = [{"x": wrap(x + dx), "c": lax.rem(c + dc, 2)} for dc, dx in pairs]
    partners += [{"y": yp}, {"y": ym}, {"zl": 1 - zl}, {"zh": zp}, {"zh": zm}]
    for where in partners:
        pl.semaphore_signal(barrier, inc=1, device_id=where, device_id_type=MESH)

    mine = x * 2 + c
    q_local = local(q_hbm, q_ref)
    stream_local = local(stream_hbm, stream_ref)
    w_local = local(w_ref.at[at(mine * block, block, block), :], ws.at[0])

    for copy in first_loads:
        copy.wait()
    values = x_ref[...].astype(F32)
    centre = jnp.mean(values, axis=-1, keepdims=True)
    offsets = values - centre
    variance = jnp.mean(offsets * offsets, axis=-1, keepdims=True)
    inv = lax.rsqrt(variance + EPS)
    inverse[...] = jnp.broadcast_to(inv, inverse.shape)
    scaled[...] = offsets * inv
    normed[...] = (scaled[...] * gain_ref[...] + bias_ref[...]).astype(BF16)

    pl.semaphore_wait(barrier, len(partners))

    chunks = [(0, sixth), (sixth, 5 * sixth)]
    spread_in = []
    for begin, size in chunks:
        for dc, dx in pairs:
            tx, tc = wrap(x + dx), lax.rem(c + dc, 2)
            piece = normed.at[:, at((tx * 2 + tc) * block + begin, size, 128)]
            spread_in.append(send(piece, spread.at[c * 4 + x, :, pl.ds(begin, size)], x=tx, c=tc))

    q_local.wait()
    for i in range(8):
        parts = [q_ref[(g * 8 + i) * tok : (g * 8 + i + 1) * tok, :].astype(F32) for g in range(4)]
        qs[0, c, i * rows_yz : (i + 1) * rows_yz, :] = jnp.concatenate(parts, axis=0).astype(BF16)
    q_d2d = {0: send(qs.at[0, c], qs.at[0, c], c=other)}
    q_down = send(qs.at[0, c], qs.at[1, c], x=xm)
    q_up = send(qs.at[0, c], qs.at[3, c], x=xp)

    spread[c * 4 + x] = normed[:, at(mine * block, block, 128)]
    base = y * 2 + zl
    own_in, zl_in = [], []
    for i, (begin, size) in enumerate(chunks):
        for copy in spread_in[i * len(pairs) : (i + 1) * len(pairs)]:
            copy.wait_recv()
        cut = pl.ds(begin, size)
        for g in range(2):
            parts = [spread[g * 4 + n, :, cut].astype(F32) for n in range(4)]
            own[g, :, cut] = jnp.concatenate(parts, axis=0).astype(BF16)
        own_in.append(local(own.at[:, :, cut], xs.at[:, at(base * rows_yz, rows_yz, rows_yz), cut]))
        for first, count in bounds:
            if begin <= first < begin + size:
                cut = pl.ds(first, count)
                zl_in.append(send(own.at[:, :, cut], xs.at[:, at(base * rows_yz, rows_yz, rows_yz), cut], zl=1 - zl))

    def w_rows(i, begin=0, size=block):
        return w_ref.at[at((i * 2 + c) * block + begin, size, size), :]

    w_down = send(w_rows(xm), ws.at[1], x=xm)
    w_up = send(w_rows(xp), ws.at[3], x=xp)
    half_w = block // 2

    y_up, y_down, relay_up, relay_down = {}, {}, {}, {}

    def y_rows(i):
        return at(i * 2 * rows_yz, 2 * rows_yz, 2 * rows_yz)

    def y_first(j):
        if j < 2:
            own_in[j].wait()
        zl_in[j].wait_recv()
        piece = xs.at[:, y_rows(y), sl[j]]
        y_up[j] = send(piece, piece, y=yp)
        y_down[j] = send(piece, piece, y=ym)

    def y_relay_up(j):
        y_up[j].wait_recv()
        piece = xs.at[0, y_rows(ym), sl[j]]
        relay_up[j] = send(piece, piece, y=yp)

    def y_relay_down(j):
        y_down[j].wait_recv()
        piece = xs.at[1, y_rows(yp), sl[j]]
        relay_down[j] = send(piece, piece, y=ym)

    units = [(k, first * sixth, size * sixth) for k, first, size in UNITS]

    def rows_of(u, q, h, base=0):
        _, begin, size = units[u]
        return at(base + begin + q * (size // 4) + h * (size // 8), size // 8, 16)

    ring = {}

    def prepare(j):
        begin, size = bounds[j]
        if not j:
            q_d2d[0].wait_recv()
        relay_up[j].wait_recv()
        relay_down[j].wait_recv()
        for g in range(2):
            xt[g, pl.ds(begin, size), :] = xs[g, :, pl.ds(begin, size)].T

    arrived = []

    def product(u):
        k, begin, size = units[u]
        if k and k not in arrived:
            arrived.append(k)
            q_d2d[k].wait_recv()
        piece = min(size, 2 * sixth)
        if size % piece:
            piece = sixth
        for first in range(begin, begin + size, piece):
            rows = pl.ds(first, piece)
            gs[k, rows, :] = (
                jnp.dot(xt[0, rows, :], qs[k, 0], preferred_element_type=F32)
                + jnp.dot(xt[1, rows, :], qs[k, 1], preferred_element_type=F32)
            ).astype(BF16)
        for d in range(2):
            ring[u, d, 0] = send(gs.at[k, rows_of(u, wrap(zh + (-1, 1)[d]), d), :], slot(u, d, 0), zh=(zp, zm)[d])

    def slot(u, d, s):
        k, begin, size = units[u]
        return rsb.at[k, d, s, pl.ds(begin // 8, size // 8), :]

    def source(k):
        return wrap(x - k) * 2 + c

    def rs_step(u, s, d):
        k, begin, size = units[u]
        ring[u, d, s - 1].wait_recv()
        sign = (-1, 1)[d]
        mine_part = gs[k, rows_of(u, wrap(zh + sign * (s + 1)), d), :].astype(F32)
        here = slot(u, d, s - 1)
        total = (here[...].astype(F32) + mine_part).astype(BF16)
        if s < 3:
            here[...] = total
            ring[u, d, s] = send(here, slot(u, d, s), zh=(zp, zm)[d])
        elif k == 0:
            out[rows_of(u, zh, d, mine * block), :] = total
        else:
            fin[k, pl.ds(begin // 4 + d * (size // 8), size // 8), :] = total

    def across(u):
        k, begin, size = units[u]
        landing = at(mine * block + begin + zh * (size // 4), size // 4, 32)
        ring[u, "x"] = send(fin.at[k, pl.ds(begin // 4, size // 4), :], out.at[landing, :], x=wrap(x + k))

    crossed = []

    def ag_step(u, s, d):
        k, begin, size = units[u]
        if s:
            ring[u, d, "a", s - 1].wait_recv()
        elif k and u not in crossed:
            crossed.append(u)
            ring[u, "x"].wait_recv()
        rows = out.at[rows_of(u, wrap(zh + (-1, 1)[d] * s), d, source(k) * block), :]
        ring[u, d, "a", s] = send(rows, rows, zh=(zp, zm)[d])

    def to_partner(u):
        k, begin, size = units[u]
        for d in range(2):
            ring[u, d, "a", 2].wait_recv()
        whole = at(source(k) * block + begin, size, 128)
        ring[u, "c"] = send(out.at[whole, :], out.at[whole, :], c=other)

    def finish(u):
        ring[u, "c"].wait_recv()

    q_relay, w_relay = {}, {}

    half = group // 2

    def q_forward_down():
        q_down.wait_recv()
        q_relay["down"] = send(qs.at[1, c, pl.ds(0, half), :], qs.at[2, c, pl.ds(0, half), :], x=xm)
        q_d2d[1] = send(qs.at[1, c], qs.at[1, c], c=other)

    def q_forward_up():
        q_up.wait_recv()
        q_relay["up"] = send(qs.at[3, c, pl.ds(half, half), :], qs.at[2, c, pl.ds(half, half), :], x=xp)
        q_d2d[3] = send(qs.at[3, c], qs.at[3, c], c=other)

    def w_first():
        w_relay["up"] = send(w_rows(xo, 0, half_w), wrelay.at[0], x=xp)
        w_relay["down"] = send(w_rows(xo, half_w, half_w), wrelay.at[1], x=xm)

    def q_last():
        q_relay["down"].wait_recv()
        q_relay["up"].wait_recv()
        q_d2d[2] = send(qs.at[2, c], qs.at[2, c], c=other)

    w_second = {}

    def w_forward_up():
        w_relay["up"].wait_recv()
        w_second["up"] = send(wrelay.at[0], ws.at[2, pl.ds(0, half_w), :], x=xp)

    def w_forward_down():
        w_relay["down"].wait_recv()
        w_second["down"] = send(wrelay.at[1], ws.at[2, pl.ds(half_w, half_w), :], x=xm)

    term_sent = {}

    def terms(dy):
        if dy == 2:
            w_local.wait()
            w_down.wait_recv()
            w_up.wait_recv()
            w_second["up"].wait_recv()
            w_second["down"].wait_recv()
        part = block // 3
        for g in range(2):
            for n in range(3):
                total = None
                for k in range(4):
                    piece = lax.dot_general(
                        qs[k, g, y_rows(wrap(y + dy)), :],
                        ws[k, pl.ds(n * part, part), :],
                        (((1,), (1,)), ((), ())),
                        preferred_element_type=F32,
                    )
                    total = piece if total is None else total + piece
                if dy:
                    tsend[dy - 1, g, :, pl.ds(n * part, part)] = total.astype(BF16)
                else:
                    tsum[g, :, pl.ds(n * part, part)] = total
        if dy == 2:
            term_sent["a0"] = send(tsend.at[1, 0], trecv.at[0], y=yp)
            term_sent["a1"] = send(tsend.at[1, 1], trecv.at[1], y=ym)
        elif dy == 1:
            term_sent["d1"] = send(tsend.at[0, 1], trecv.at[2], y=yp)
        elif dy == 3:
            term_sent["d0"] = send(tsend.at[2, 0], trecv.at[3], y=ym)

    def terms_relay_up():
        term_sent["a0"].wait_recv()
        trecv[0] = (trecv[0].astype(F32) + tsend[0, 0].astype(F32)).astype(BF16)
        term_sent["b0"] = send(trecv.at[0], trecv.at[4], y=yp)

    def terms_relay_down():
        term_sent["a1"].wait_recv()
        trecv[1] = (trecv[1].astype(F32) + tsend[2, 1].astype(F32)).astype(BF16)
        term_sent["b1"] = send(trecv.at[1], trecv.at[5], y=ym)

    def half_rows(which):
        return at(which * rows_yz, rows_yz, rows_yz)

    def terms_sum():
        term_sent["b0"].wait_recv()
        term_sent["d0"].wait_recv()
        term_sent["b1"].wait_recv()
        term_sent["d1"].wait_recv()
        for g, (i, j) in enumerate(((4, 3), (5, 2))):
            far = half_rows(1 - zl)
            tzs[g] = (tsum[g, far, :] + trecv[i, far, :].astype(F32) + trecv[j, far, :].astype(F32)).astype(BF16)
        term_sent["z"] = send(tzs, tzr, zl=1 - zl)

    def terms_back():
        term_sent["z"].wait_recv()
        for g, (i, j) in enumerate(((4, 3), (5, 2))):
            near = half_rows(zl)
            total = (
                tsum[g, near, :]
                + trecv[i, near, :].astype(F32)
                + trecv[j, near, :].astype(F32)
                + tzr[g].astype(F32)
            )
            for i in range(4):
                back[g * 4 + i] = total[i * tok : (i + 1) * tok, :].astype(BF16)
        for dc, dx in pairs:
            tx, tc = wrap(x + dx), lax.rem(c + dc, 2)
            term_sent[dc, dx] = send(back.at[tc * 4 + tx], ngf.at[mine], x=tx, c=tc)
        ngf[mine] = back[c * 4 + x]

    def norm_backward():
        for pair in pairs:
            term_sent[pair].wait_recv()
        grad = jnp.concatenate([ngf[i].astype(F32) for i in range(8)], axis=1)
        weighted = grad * gain_ref[...]
        scaled_now = scaled[...]
        first = jnp.mean(weighted, axis=-1, keepdims=True)
        second = jnp.mean(weighted * scaled_now, axis=-1, keepdims=True)
        stream_local.wait()
        result = stream_ref[...].astype(F32) + inverse[:, 0:1] * (weighted - first - scaled_now * second)
        dx_ref[...] = result.astype(BF16)

    actions = {
        "yf": y_first, "yu": y_relay_up, "yd": y_relay_down, "prep": prepare, "P": product, "R": rs_step,
        "X": across, "A": ag_step, "D": to_partner, "F": finish, "qd": q_forward_down, "qu": q_forward_up,
        "ql": q_last, "wr": w_first, "wfu": w_forward_up, "wfd": w_forward_down, "T": terms,
        "tr0": terms_relay_up, "tr1": terms_relay_down, "ts": terms_sum, "tb": terms_back, "nb": norm_backward,
    }
    for name, *rest in ORDER:
        actions[name](*rest)

    for copy in copies:
        copy.wait_send()


N_COPIES = 224
N_LOCAL = 8

ORDER = [
    ("yf", 0), ("yf", 1), ("yu", 0), ("yd", 0), ("yf", 2), ("yu", 1), ("yd", 1), ("yf", 3), ("prep", 0), ("P", 0),
    ("qd",), ("yu", 2), ("yd", 2), ("yf", 4), ("prep", 1), ("qu",), ("wr",), ("P", 1), ("P", 2), ("R", 0, 1, 0),
    ("R", 0, 1, 1), ("yu", 3), ("yd", 3), ("yf", 5), ("P", 3), ("prep", 2), ("R", 1, 1, 0), ("R", 1, 1, 1),
    ("yu", 4), ("yd", 4), ("R", 2, 1, 0), ("R", 2, 1, 1), ("R", 0, 2, 0), ("R", 0, 2, 1), ("prep", 3), ("P", 4),
    ("R", 3, 1, 0), ("R", 3, 1, 1), ("R", 1, 2, 0), ("R", 1, 2, 1), ("yu", 5), ("yd", 5), ("prep", 4),
    ("R", 2, 2, 0), ("R", 2, 2, 1), ("R", 0, 3, 0), ("R", 0, 3, 1), ("A", 0, 0, 0), ("A", 0, 0, 1), ("R", 4, 1, 0),
    ("R", 4, 1, 1), ("prep", 5), ("P", 5), ("P", 6), ("P", 7), ("R", 3, 2, 0), ("R", 3, 2, 1), ("R", 1, 3, 0),
    ("R", 1, 3, 1), ("R", 4, 2, 0), ("R", 4, 2, 1), ("R", 2, 3, 0), ("R", 2, 3, 1), ("X", 2), ("A", 1, 0, 0),
    ("A", 1, 0, 1), ("A", 0, 1, 0), ("A", 0, 1, 1), ("R", 5, 1, 0), ("R", 5, 1, 1), ("R", 6, 1, 0), ("R", 6, 1, 1),
    ("ql",), ("R", 7, 1, 0), ("R", 7, 1, 1), ("P", 8), ("P", 9), ("R", 3, 3, 0), ("R", 3, 3, 1), ("X", 3),
    ("R", 4, 3, 0), ("R", 4, 3, 1), ("A", 4, 0, 0), ("A", 4, 0, 1), ("A", 1, 1, 0), ("A", 1, 1, 1), ("A", 0, 2, 0),
    ("wfd",), ("A", 0, 2, 1), ("R", 5, 2, 0), ("R", 5, 2, 1), ("wfu",), ("A", 3, 0, 0), ("A", 3, 0, 1),
    ("A", 2, 0, 0), ("A", 2, 0, 1), ("R", 6, 2, 0), ("R", 6, 2, 1), ("R", 7, 2, 0), ("R", 7, 2, 1), ("R", 8, 1, 0),
    ("R", 8, 1, 1), ("R", 9, 1, 0), ("R", 9, 1, 1), ("A", 4, 1, 0), ("A", 4, 1, 1), ("A", 1, 2, 0), ("T", 2),
    ("T", 1), ("T", 3), ("T", 0), ("R", 5, 3, 0), ("R", 5, 3, 1), ("R", 6, 3, 0), ("R", 6, 3, 1), ("X", 6),
    ("R", 7, 3, 0), ("R", 7, 3, 1), ("X", 7), ("A", 5, 0, 0), ("A", 5, 0, 1), ("A", 2, 1, 0), ("A", 2, 1, 1),
    ("A", 3, 1, 0), ("A", 3, 1, 1), ("A", 1, 2, 1), ("D", 0), ("R", 8, 2, 0), ("R", 8, 2, 1), ("F", 0), ("tr0",),
    ("tr1",), ("R", 9, 2, 0), ("R", 9, 2, 1), ("A", 4, 2, 0), ("A", 4, 2, 1), ("A", 6, 0, 0), ("A", 6, 0, 1),
    ("A", 7, 0, 0), ("A", 7, 0, 1), ("A", 5, 1, 1), ("A", 5, 1, 0), ("A", 2, 2, 1), ("A", 2, 2, 0), ("A", 3, 2, 1),
    ("A", 3, 2, 0), ("D", 1), ("F", 1), ("R", 8, 3, 0), ("R", 8, 3, 1), ("X", 8), ("R", 9, 3, 0), ("R", 9, 3, 1),
    ("X", 9), ("D", 4), ("F", 4), ("A", 6, 1, 0), ("A", 6, 1, 1), ("A", 8, 0, 0), ("A", 8, 0, 1), ("ts",),
    ("A", 9, 0, 0), ("A", 9, 0, 1), ("A", 7, 1, 0), ("A", 7, 1, 1), ("A", 5, 2, 0), ("A", 5, 2, 1), ("D", 2),
    ("D", 3), ("F", 2), ("F", 3), ("A", 6, 2, 0), ("A", 6, 2, 1), ("A", 8, 1, 0), ("A", 8, 1, 1), ("tb",),
    ("A", 9, 1, 0), ("A", 9, 1, 1), ("A", 7, 2, 0), ("A", 7, 2, 1), ("D", 5), ("nb",), ("F", 5), ("D", 6),
    ("A", 8, 2, 0), ("A", 8, 2, 1), ("F", 6), ("A", 9, 2, 0), ("A", 9, 2, 1), ("D", 7), ("D", 8), ("F", 7), ("F", 8),
    ("D", 9), ("F", 9),
]
UNITS = [(0, 0, 1), (0, 1, 1), (1, 0, 2), (3, 0, 2), (0, 2, 2), (0, 4, 2), (1, 2, 4), (3, 2, 4), (2, 0, 3), (2, 3, 3)]


def shards(inputs, norm_gain, norm_bias, query_grad, stream_grad, query_weight):
    tok, width = inputs.shape
    rows, cols = query_grad.shape
    block = width // 8
    vmem = pl.BlockSpec(memory_space=pltpu.VMEM)
    hbm = pl.BlockSpec(memory_space=pltpu.HBM)
    return pl.pallas_call(
        kernel,
        out_shape=(
            pltpu.VMEM((tok, width), BF16),
            pltpu.VMEM((width, cols), BF16),
        ),
        in_specs=[hbm] * 6,
        out_specs=(vmem, vmem),
        scratch_shapes=[
            pltpu.VMEM((tok, width), BF16),
            pltpu.VMEM((1, width), F32),
            pltpu.VMEM((1, width), F32),
            pltpu.VMEM((rows, cols), BF16),
            pltpu.VMEM((tok, width), BF16),
            pltpu.VMEM((tok, width), F32),
            pltpu.VMEM((tok, 128), F32),
            pltpu.VMEM((tok, width), BF16),
            pltpu.VMEM((8, tok, block), BF16),
            pltpu.VMEM((2, 4 * tok, block), BF16),
            pltpu.VMEM((2, rows, block), BF16),
            pltpu.VMEM((2, block, rows), BF16),
            pltpu.VMEM((4, 2, rows, cols), BF16),
            pltpu.VMEM((4, block, cols), BF16),
            pltpu.VMEM((2, block // 2, cols), BF16),
            pltpu.VMEM((4, block, cols), BF16),
            pltpu.VMEM((4, 2, 3, block // 8, cols), BF16),
            pltpu.VMEM((4, block // 4, cols), BF16),
            pltpu.VMEM((3, 2, 8 * tok, block), BF16),
            pltpu.VMEM((6, 8 * tok, block), BF16),
            pltpu.VMEM((2, 8 * tok, block), F32),
            pltpu.VMEM((2, 4 * tok, block), BF16),
            pltpu.VMEM((2, 4 * tok, block), BF16),
            pltpu.VMEM((8, tok, block), BF16),
            pltpu.VMEM((8, tok, block), BF16),
            pltpu.SemaphoreType.DMA((N_COPIES,)),
            pltpu.SemaphoreType.DMA((N_COPIES,)),
            pltpu.SemaphoreType.DMA((N_LOCAL,)),
        ],
        compiler_params=pltpu.CompilerParams(
            collective_id=0, has_side_effects=True, vmem_limit_bytes=57 * 1024 * 1024
        ),
    )(inputs, norm_gain.reshape(1, width), norm_bias.reshape(1, width), query_grad, stream_grad, query_weight)


def solution(mesh):
    torus = Mesh(mesh.devices.reshape(4, 2, 4, 4, 2), ALL)
    return jax.shard_map(
        shards,
        mesh=torus,
        in_specs=(P(ALL, None), P(), P(), P(DP, TENSOR), P(ALL, None), P(None, TENSOR)),
        out_specs=(P(ALL, None), P(None, TENSOR)),
        check_vma=False,
    )
```

```python
import jax
import jax.numpy as jnp
from jax import lax
from jax.experimental import pallas as pl
from jax.experimental.pallas import tpu as pltpu
from jax.sharding import Mesh
from jax.sharding import PartitionSpec as P

MESH = pl.DeviceIdType.MESH
DP = ("zh", "c")
TENSOR = ("x", "y", "zl")
ALL = DP + TENSOR
EPS = 1e-05

F32 = jnp.float32
BF16 = jnp.bfloat16


def kernel(
    x_hbm, gain_hbm, bias_hbm, q_hbm, stream_hbm, w_ref, dx_ref, out,
    x_ref, gain_ref, bias_ref, q_ref, stream_ref,
    scaled, inverse, normed, spread, own, xs, xt, qs, ws, wrelay, gs, rsb, fin,
    tsend, trecv, tsum, tzs, tzr, back, ngf,
    send_sem, recv_sem, local_sem,
):
    zh, c, x, y, zl = [lax.axis_index(name) for name in ALL]
    tok, width = x_ref.shape
    block = width // 8
    cols = q_ref.shape[1]
    rows_yz = 4 * tok
    group = 8 * rows_yz
    sixth = block // 6
    bounds = [(i * sixth, sixth) for i in range(6)]
    sl = [pl.ds(*bound) for bound in bounds]

    def wrap(value):
        return lax.rem(value + 8, 4)

    xm, xp, xo = wrap(x - 1), wrap(x + 1), wrap(x + 2)
    ym, yp, yo = wrap(y - 1), wrap(y + 1), wrap(y + 2)
    zm, zp = wrap(zh - 1), wrap(zh + 1)
    other = 1 - c

    def at(offset, size, unit):
        return pl.ds(pl.multiple_of(offset, unit), size)

    copies = []
    locals_ = []

    def send(src, dst, **where):
        i = len(copies)
        copy = pltpu.make_async_remote_copy(
            src_ref=src,
            dst_ref=dst,
            send_sem=send_sem.at[i],
            recv_sem=recv_sem.at[i],
            device_id=where,
            device_id_type=MESH,
        )
        copy.start()
        copies.append(copy)
        return copy

    def local(src, dst):
        copy = pltpu.make_async_copy(src, dst, local_sem.at[len(locals_)])
        copy.start()
        locals_.append(copy)
        return copy

    first_loads = [local(x_hbm, x_ref), local(gain_hbm, gain_ref), local(bias_hbm, bias_ref)]

    pairs = [(dc, dx) for dc in range(2) for dx in range(4) if dc or dx]
    barrier = pltpu.get_barrier_semaphore()
    partners = [{"x": wrap(x + dx), "c": lax.rem(c + dc, 2)} for dc, dx in pairs]
    partners += [{"y": yp}, {"y": ym}, {"zl": 1 - zl}, {"zh": zp}, {"zh": zm}]
    for where in partners:
        pl.semaphore_signal(barrier, inc=1, device_id=where, device_id_type=MESH)

    mine = x * 2 + c
    q_local = local(q_hbm, q_ref)
    stream_local = local(stream_hbm, stream_ref)
    w_local = local(w_ref.at[at(mine * block, block, block), :], ws.at[0])

    for copy in first_loads:
        copy.wait()
    values = x_ref[...].astype(F32)
    centre = jnp.mean(values, axis=-1, keepdims=True)
    offsets = values - centre
    variance = jnp.mean(offsets * offsets, axis=-1, keepdims=True)
    inv = lax.rsqrt(variance + EPS)
    inverse[...] = jnp.broadcast_to(inv, inverse.shape)
    scaled[...] = offsets * inv
    normed[...] = (scaled[...] * gain_ref[...] + bias_ref[...]).astype(BF16)

    pl.semaphore_wait(barrier, len(partners))

    chunks = [(0, sixth), (sixth, 5 * sixth)]
    spread_in = []
    for begin, size in chunks:
        for dc, dx in pairs:
            tx, tc = wrap(x + dx), lax.rem(c + dc, 2)
            piece = normed.at[:, at((tx * 2 + tc) * block + begin, size, 128)]
            spread_in.append(send(piece, spread.at[c * 4 + x, :, pl.ds(begin, size)], x=tx, c=tc))

    q_local.wait()
    for i in range(8):
        parts = [q_ref[(g * 8 + i) * tok : (g * 8 + i + 1) * tok, :].astype(F32) for g in range(4)]
        qs[0, c, i * rows_yz : (i + 1) * rows_yz, :] = jnp.concatenate(parts, axis=0).astype(BF16)
    q_d2d = {0: send(qs.at[0, c], qs.at[0, c], c=other)}
    q_down = send(qs.at[0, c], qs.at[1, c], x=xm)
    q_up = send(qs.at[0, c], qs.at[3, c], x=xp)

    spread[c * 4 + x] = normed[:, at(mine * block, block, 128)]
    base = y * 2 + zl
    own_in, zl_in = [], []
    for i, (begin, size) in enumerate(chunks):
        for copy in spread_in[i * len(pairs) : (i + 1) * len(pairs)]:
            copy.wait_recv()
        cut = pl.ds(begin, size)
        for g in range(2):
            parts = [spread[g * 4 + n, :, cut].astype(F32) for n in range(4)]
            own[g, :, cut] = jnp.concatenate(parts, axis=0).astype(BF16)
        own_in.append(local(own.at[:, :, cut], xs.at[:, at(base * rows_yz, rows_yz, rows_yz), cut]))
        for first, count in bounds:
            if begin <= first < begin + size:
                cut = pl.ds(first, count)
                zl_in.append(send(own.at[:, :, cut], xs.at[:, at(base * rows_yz, rows_yz, rows_yz), cut], zl=1 - zl))

    def w_rows(i, begin=0, size=block):
        return w_ref.at[at((i * 2 + c) * block + begin, size, size), :]

    w_down = send(w_rows(xm), ws.at[1], x=xm)
    w_up = send(w_rows(xp), ws.at[3], x=xp)
    half_w = block // 2

    y_up, y_down, relay_up, relay_down = {}, {}, {}, {}

    def y_rows(i):
        return at(i * 2 * rows_yz, 2 * rows_yz, 2 * rows_yz)

    def y_first(j):
        if j < 2:
            own_in[j].wait()
        zl_in[j].wait_recv()
        piece = xs.at[:, y_rows(y), sl[j]]
        y_up[j] = send(piece, piece, y=yp)
        y_down[j] = send(piece, piece, y=ym)

    def y_relay_up(j):
        y_up[j].wait_recv()
        piece = xs.at[0, y_rows(ym), sl[j]]
        relay_up[j] = send(piece, piece, y=yp)

    def y_relay_down(j):
        y_down[j].wait_recv()
        piece = xs.at[1, y_rows(yp), sl[j]]
        relay_down[j] = send(piece, piece, y=ym)

    units = [(k, first * sixth, size * sixth) for k, first, size in UNITS]

    def rows_of(u, q, h, base=0):
        _, begin, size = units[u]
        return at(base + begin + q * (size // 4) + h * (size // 8), size // 8, 16)

    ring = {}

    def prepare(j):
        begin, size = bounds[j]
        if not j:
            q_d2d[0].wait_recv()
        relay_up[j].wait_recv()
        relay_down[j].wait_recv()
        for g in range(2):
            xt[g, pl.ds(begin, size), :] = xs[g, :, pl.ds(begin, size)].T

    arrived = []

    def product(u):
        k, begin, size = units[u]
        if k and k not in arrived:
            arrived.append(k)
            q_d2d[k].wait_recv()
        piece = min(size, 2 * sixth)
        if size % piece:
            piece = sixth
        for first in range(begin, begin + size, piece):
            rows = pl.ds(first, piece)
            gs[k, rows, :] = (
                jnp.dot(xt[0, rows, :], qs[k, 0], preferred_element_type=F32)
                + jnp.dot(xt[1, rows, :], qs[k, 1], preferred_element_type=F32)
            ).astype(BF16)
        for d in range(2):
            ring[u, d, 0] = send(gs.at[k, rows_of(u, wrap(zh + (-1, 1)[d]), d), :], slot(u, d, 0), zh=(zp, zm)[d])

    def slot(u, d, s):
        k, begin, size = units[u]
        return rsb.at[k, d, s, pl.ds(begin // 8, size // 8), :]

    def source(k):
        return wrap(x - k) * 2 + c

    def rs_step(u, s, d):
        k, begin, size = units[u]
        ring[u, d, s - 1].wait_recv()
        sign = (-1, 1)[d]
        mine_part = gs[k, rows_of(u, wrap(zh + sign * (s + 1)), d), :].astype(F32)
        here = slot(u, d, s - 1)
        total = (here[...].astype(F32) + mine_part).astype(BF16)
        if s < 3:
            here[...] = total
            ring[u, d, s] = send(here, slot(u, d, s), zh=(zp, zm)[d])
        elif k == 0:
            out[rows_of(u, zh, d, mine * block), :] = total
        else:
            fin[k, pl.ds(begin // 4 + d * (size // 8), size // 8), :] = total

    def across(u):
        k, begin, size = units[u]
        landing = at(mine * block + begin + zh * (size // 4), size // 4, 32)
        ring[u, "x"] = send(fin.at[k, pl.ds(begin // 4, size // 4), :], out.at[landing, :], x=wrap(x + k))

    crossed = []

    def ag_step(u, s, d):
        k, begin, size = units[u]
        if s:
            ring[u, d, "a", s - 1].wait_recv()
        elif k and u not in crossed:
            crossed.append(u)
            ring[u, "x"].wait_recv()
        rows = out.at[rows_of(u, wrap(zh + (-1, 1)[d] * s), d, source(k) * block), :]
        ring[u, d, "a", s] = send(rows, rows, zh=(zp, zm)[d])

    def to_partner(u):
        k, begin, size = units[u]
        for d in range(2):
            ring[u, d, "a", 2].wait_recv()
        whole = at(source(k) * block + begin, size, 128)
        ring[u, "c"] = send(out.at[whole, :], out.at[whole, :], c=other)

    def finish(u):
        ring[u, "c"].wait_recv()

    q_relay, w_relay = {}, {}

    half = group // 2

    def q_forward_down():
        q_down.wait_recv()
        q_relay["down"] = send(qs.at[1, c, pl.ds(0, half), :], qs.at[2, c, pl.ds(0, half), :], x=xm)
        q_d2d[1] = send(qs.at[1, c], qs.at[1, c], c=other)

    def q_forward_up():
        q_up.wait_recv()
        q_relay["up"] = send(qs.at[3, c, pl.ds(half, half), :], qs.at[2, c, pl.ds(half, half), :], x=xp)
        q_d2d[3] = send(qs.at[3, c], qs.at[3, c], c=other)

    def w_first():
        w_relay["up"] = send(w_rows(xo, 0, half_w), wrelay.at[0], x=xp)
        w_relay["down"] = send(w_rows(xo, half_w, half_w), wrelay.at[1], x=xm)

    def q_last():
        q_relay["down"].wait_recv()
        q_relay["up"].wait_recv()
        q_d2d[2] = send(qs.at[2, c], qs.at[2, c], c=other)

    w_second = {}

    def w_forward_up():
        w_relay["up"].wait_recv()
        w_second["up"] = send(wrelay.at[0], ws.at[2, pl.ds(0, half_w), :], x=xp)

    def w_forward_down():
        w_relay["down"].wait_recv()
        w_second["down"] = send(wrelay.at[1], ws.at[2, pl.ds(half_w, half_w), :], x=xm)

    term_sent = {}

    waited = []

    def terms(dy):
        if not waited:
            waited.append(True)
            w_local.wait()
            w_down.wait_recv()
            w_up.wait_recv()
            w_second["up"].wait_recv()
            w_second["down"].wait_recv()
            for k in (1, 2, 3):
                if k not in arrived:
                    arrived.append(k)
                    q_d2d[k].wait_recv()
        part = block // 3
        for g in range(2):
            for n in range(3):
                total = None
                for k in range(4):
                    piece = lax.dot_general(
                        qs[k, g, y_rows(wrap(y + dy)), :],
                        ws[k, pl.ds(n * part, part), :],
                        (((1,), (1,)), ((), ())),
                        preferred_element_type=F32,
                    )
                    total = piece if total is None else total + piece
                if dy:
                    tsend[dy - 1, g, :, pl.ds(n * part, part)] = total.astype(BF16)
                else:
                    tsum[g, :, pl.ds(n * part, part)] = total
        if dy == 2:
            term_sent["a0"] = send(tsend.at[1, 0], trecv.at[0], y=yp)
            term_sent["a1"] = send(tsend.at[1, 1], trecv.at[1], y=ym)
        elif dy == 1:
            term_sent["d1"] = send(tsend.at[0, 1], trecv.at[2], y=yp)
        elif dy == 3:
            term_sent["d0"] = send(tsend.at[2, 0], trecv.at[3], y=ym)

    def terms_relay_up():
        term_sent["a0"].wait_recv()
        trecv[0] = (trecv[0].astype(F32) + tsend[0, 0].astype(F32)).astype(BF16)
        term_sent["b0"] = send(trecv.at[0], trecv.at[4], y=yp)

    def terms_relay_down():
        term_sent["a1"].wait_recv()
        trecv[1] = (trecv[1].astype(F32) + tsend[2, 1].astype(F32)).astype(BF16)
        term_sent["b1"] = send(trecv.at[1], trecv.at[5], y=ym)

    def half_rows(which):
        return at(which * rows_yz, rows_yz, rows_yz)

    def terms_sum():
        term_sent["b0"].wait_recv()
        term_sent["d0"].wait_recv()
        term_sent["b1"].wait_recv()
        term_sent["d1"].wait_recv()
        for g, (i, j) in enumerate(((4, 3), (5, 2))):
            far = half_rows(1 - zl)
            tzs[g] = (tsum[g, far, :] + trecv[i, far, :].astype(F32) + trecv[j, far, :].astype(F32)).astype(BF16)
        term_sent["z"] = send(tzs, tzr, zl=1 - zl)

    def terms_back():
        term_sent["z"].wait_recv()
        for g, (i, j) in enumerate(((4, 3), (5, 2))):
            near = half_rows(zl)
            total = (
                tsum[g, near, :]
                + trecv[i, near, :].astype(F32)
                + trecv[j, near, :].astype(F32)
                + tzr[g].astype(F32)
            )
            for i in range(4):
                back[g * 4 + i] = total[i * tok : (i + 1) * tok, :].astype(BF16)
        for dc, dx in pairs:
            tx, tc = wrap(x + dx), lax.rem(c + dc, 2)
            term_sent[dc, dx] = send(back.at[tc * 4 + tx], ngf.at[mine], x=tx, c=tc)
        ngf[mine] = back[c * 4 + x]

    def norm_backward():
        for pair in pairs:
            term_sent[pair].wait_recv()
        grad = jnp.concatenate([ngf[i].astype(F32) for i in range(8)], axis=1)
        weighted = grad * gain_ref[...]
        scaled_now = scaled[...]
        first = jnp.mean(weighted, axis=-1, keepdims=True)
        second = jnp.mean(weighted * scaled_now, axis=-1, keepdims=True)
        stream_local.wait()
        result = stream_ref[...].astype(F32) + inverse[:, 0:1] * (weighted - first - scaled_now * second)
        dx_ref[...] = result.astype(BF16)

    actions = {
        "yf": y_first, "yu": y_relay_up, "yd": y_relay_down, "prep": prepare, "P": product, "R": rs_step,
        "X": across, "A": ag_step, "D": to_partner, "F": finish, "qd": q_forward_down, "qu": q_forward_up,
        "ql": q_last, "wr": w_first, "wfu": w_forward_up, "wfd": w_forward_down, "T": terms,
        "tr0": terms_relay_up, "tr1": terms_relay_down, "ts": terms_sum, "tb": terms_back, "nb": norm_backward,
    }
    for name, *rest in ORDER:
        actions[name](*rest)

    for copy in copies:
        copy.wait_send()


N_COPIES = 256
N_LOCAL = 8

ORDER = [
    ("yf", 0), ("yf", 1), ("yu", 0), ("yd", 0), ("yf", 2), ("yu", 1), ("yd", 1), ("yf", 3), ("prep", 0), ("P", 0),
    ("yu", 2), ("yd", 2), ("yf", 4), ("prep", 1), ("qd",), ("qu",), ("wr",), ("P", 1), ("R", 0, 1, 0),
    ("R", 0, 1, 1), ("yu", 3), ("yd", 3), ("yf", 5), ("P", 2), ("P", 4), ("prep", 2), ("P", 3), ("P", 5),
    ("R", 1, 1, 0), ("R", 1, 1, 1), ("R", 0, 2, 0), ("R", 0, 2, 1), ("yu", 4), ("yd", 4), ("R", 2, 1, 0),
    ("R", 2, 1, 1), ("prep", 3), ("P", 6), ("R", 3, 1, 0), ("R", 3, 1, 1), ("R", 4, 1, 0), ("R", 4, 1, 1),
    ("R", 5, 1, 0), ("R", 5, 1, 1), ("R", 1, 2, 0), ("yu", 5), ("yd", 5), ("R", 1, 2, 1), ("R", 0, 3, 0),
    ("R", 0, 3, 1), ("A", 0, 0, 0), ("A", 0, 0, 1), ("prep", 4), ("R", 2, 2, 0), ("R", 2, 2, 1), ("R", 6, 1, 0),
    ("R", 6, 1, 1), ("prep", 5), ("P", 7), ("P", 8), ("P", 9), ("A", 0, 1, 0), ("A", 0, 1, 1), ("R", 3, 2, 0),
    ("R", 3, 2, 1), ("R", 4, 2, 0), ("R", 4, 2, 1), ("R", 5, 2, 0), ("R", 5, 2, 1), ("R", 6, 2, 0), ("R", 6, 2, 1),
    ("R", 1, 3, 0), ("R", 1, 3, 1), ("A", 1, 0, 0), ("A", 1, 0, 1), ("R", 7, 1, 0), ("R", 7, 1, 1), ("R", 2, 3, 0),
    ("R", 2, 3, 1), ("X", 2), ("R", 8, 1, 0), ("R", 8, 1, 1), ("ql",), ("R", 9, 1, 0), ("R", 9, 1, 1), ("P", 10),
    ("P", 11), ("A", 0, 2, 0), ("A", 0, 2, 1), ("R", 3, 3, 0), ("R", 3, 3, 1), ("X", 3), ("R", 4, 3, 0),
    ("R", 4, 3, 1), ("X", 4), ("R", 5, 3, 0), ("R", 5, 3, 1), ("X", 5), ("R", 6, 3, 0), ("R", 6, 3, 1),
    ("A", 6, 0, 0), ("A", 6, 0, 1), ("A", 1, 1, 0), ("A", 1, 1, 1), ("wfu",), ("wfd",), ("R", 7, 2, 0),
    ("R", 7, 2, 1), ("A", 2, 0, 0), ("A", 2, 0, 1), ("A", 3, 0, 0), ("A", 3, 0, 1), ("A", 4, 0, 0), ("A", 4, 0, 1),
    ("A", 5, 0, 0), ("A", 5, 0, 1), ("R", 8, 2, 0), ("R", 8, 2, 1), ("R", 9, 2, 0), ("R", 9, 2, 1), ("R", 10, 1, 0),
    ("R", 10, 1, 1), ("R", 11, 1, 0), ("R", 11, 1, 1), ("D", 0), ("T", 2), ("T", 1), ("T", 3), ("A", 2, 1, 0),
    ("A", 2, 1, 1), ("A", 3, 1, 0), ("A", 3, 1, 1), ("A", 4, 1, 0), ("A", 4, 1, 1), ("A", 5, 1, 0), ("A", 5, 1, 1),
    ("A", 6, 1, 0), ("A", 6, 1, 1), ("T", 0), ("A", 1, 2, 0), ("A", 1, 2, 1), ("R", 7, 3, 0), ("R", 7, 3, 1),
    ("A", 7, 0, 0), ("A", 7, 0, 1), ("R", 8, 3, 0), ("R", 8, 3, 1), ("X", 8), ("R", 9, 3, 0), ("R", 9, 3, 1),
    ("X", 9), ("F", 0), ("R", 10, 2, 0), ("tr0",), ("tr1",), ("R", 10, 2, 1), ("R", 11, 2, 0), ("R", 11, 2, 1),
    ("A", 2, 2, 0), ("A", 2, 2, 1), ("A", 3, 2, 0), ("A", 3, 2, 1), ("A", 8, 0, 0), ("A", 8, 0, 1), ("A", 4, 2, 0),
    ("A", 9, 0, 0), ("A", 9, 0, 1), ("A", 4, 2, 1), ("A", 5, 2, 0), ("A", 5, 2, 1), ("A", 6, 2, 0), ("A", 6, 2, 1),
    ("D", 1), ("A", 7, 1, 0), ("A", 7, 1, 1), ("F", 1), ("R", 10, 3, 0), ("R", 10, 3, 1), ("X", 10), ("R", 11, 3, 0),
    ("R", 11, 3, 1), ("X", 11), ("D", 2), ("D", 3), ("F", 2), ("F", 3), ("A", 8, 1, 0), ("A", 8, 1, 1),
    ("A", 10, 0, 0), ("ts",), ("A", 10, 0, 1), ("A", 11, 0, 0), ("A", 11, 0, 1), ("A", 9, 1, 1), ("A", 9, 1, 0),
    ("D", 4), ("D", 5), ("F", 4), ("D", 6), ("F", 5), ("A", 7, 2, 0), ("A", 7, 2, 1), ("F", 6), ("A", 8, 2, 0),
    ("A", 8, 2, 1), ("A", 10, 1, 0), ("A", 10, 1, 1), ("A", 11, 1, 0), ("A", 11, 1, 1), ("A", 9, 2, 0),
    ("A", 9, 2, 1), ("tb",), ("D", 7), ("F", 7), ("D", 8), ("A", 10, 2, 0), ("A", 10, 2, 1), ("F", 8),
    ("A", 11, 2, 0), ("A", 11, 2, 1), ("nb",), ("D", 9), ("D", 10), ("F", 9), ("F", 10), ("D", 11), ("F", 11),
]
UNITS = [(0, 0, 1), (0, 1, 1), (1, 0, 1), (3, 0, 1), (1, 1, 1), (3, 1, 1), (0, 2, 2), (0, 4, 2), (1, 2, 4), (3, 2, 4), (2, 0, 3), (2, 3, 3)]


def write_out(small, large, small_out, large_out, sem):
    rows = large.shape[0] // 4
    copies = [pltpu.make_async_copy(small, small_out, sem.at[4])]
    for i in range(4):
        cut = pl.ds(i * rows, rows)
        copies.append(pltpu.make_async_copy(large.at[cut, :], large_out.at[cut, :], sem.at[i]))
    for copy in copies:
        copy.start()
    for copy in copies:
        copy.wait()


def shards(inputs, norm_gain, norm_bias, query_grad, stream_grad, query_weight):
    tok, width = inputs.shape
    rows, cols = query_grad.shape
    block = width // 8
    vmem = pl.BlockSpec(memory_space=pltpu.VMEM)
    hbm = pl.BlockSpec(memory_space=pltpu.HBM)
    results = pl.pallas_call(
        kernel,
        out_shape=(
            pltpu.VMEM((tok, width), BF16),
            pltpu.VMEM((width, cols), BF16),
        ),
        in_specs=[hbm] * 6,
        out_specs=(vmem, vmem),
        scratch_shapes=[
            pltpu.VMEM((tok, width), BF16),
            pltpu.VMEM((1, width), F32),
            pltpu.VMEM((1, width), F32),
            pltpu.VMEM((rows, cols), BF16),
            pltpu.VMEM((tok, width), BF16),
            pltpu.VMEM((tok, width), F32),
            pltpu.VMEM((tok, 128), F32),
            pltpu.VMEM((tok, width), BF16),
            pltpu.VMEM((8, tok, block), BF16),
            pltpu.VMEM((2, 4 * tok, block), BF16),
            pltpu.VMEM((2, rows, block), BF16),
            pltpu.VMEM((2, block, rows), BF16),
            pltpu.VMEM((4, 2, rows, cols), BF16),
            pltpu.VMEM((4, block, cols), BF16),
            pltpu.VMEM((2, block // 2, cols), BF16),
            pltpu.VMEM((4, block, cols), BF16),
            pltpu.VMEM((4, 2, 3, block // 8, cols), BF16),
            pltpu.VMEM((4, block // 4, cols), BF16),
            pltpu.VMEM((3, 2, 8 * tok, block), BF16),
            pltpu.VMEM((6, 8 * tok, block), BF16),
            pltpu.VMEM((2, 8 * tok, block), F32),
            pltpu.VMEM((2, 4 * tok, block), BF16),
            pltpu.VMEM((2, 4 * tok, block), BF16),
            pltpu.VMEM((8, tok, block), BF16),
            pltpu.VMEM((8, tok, block), BF16),
            pltpu.SemaphoreType.DMA((N_COPIES,)),
            pltpu.SemaphoreType.DMA((N_COPIES,)),
            pltpu.SemaphoreType.DMA((N_LOCAL,)),
        ],
        compiler_params=pltpu.CompilerParams(
            collective_id=0, has_side_effects=True, vmem_limit_bytes=57 * 1024 * 1024
        ),
    )(inputs, norm_gain.reshape(1, width), norm_bias.reshape(1, width), query_grad, stream_grad, query_weight)
    anywhere = pl.BlockSpec(memory_space=pl.ANY)
    return pl.pallas_call(
        write_out,
        out_shape=(
            jax.ShapeDtypeStruct((tok, width), BF16),
            jax.ShapeDtypeStruct((width, cols), BF16),
        ),
        in_specs=[anywhere] * 2,
        out_specs=(hbm, hbm),
        scratch_shapes=[pltpu.SemaphoreType.DMA((5,))],
        compiler_params=pltpu.CompilerParams(vmem_limit_bytes=1024 * 1024),
    )(*[pltpu.with_memory_space_constraint(result, pltpu.VMEM) for result in results])


def solution(mesh):
    torus = Mesh(mesh.devices.reshape(4, 2, 4, 4, 2), ALL)
    return jax.shard_map(
        shards,
        mesh=torus,
        in_specs=(P(ALL, None), P(), P(), P(DP, TENSOR), P(ALL, None), P(None, TENSOR)),
        out_specs=(P(ALL, None), P(None, TENSOR)),
        check_vma=False,
    )
```
